32 devices in a mesh: rep: 1 (over z), tp: 4 (over y), sp: 8 (over x, core).
Axes of the slice: x: 4, y: 4, z: 1, core: 2. Of those that a mesh axis runs over, the one named last changes fastest.
The devices are a block of a 4x4x8 slice.
Arguments:
- x_in: bfloat16 [8192, 4096], P(('rep', 'sp'))
- positions: int32 [8192], P(('rep', 'sp'))
- segments: int32 [8192], P(('rep', 'sp'))
- gain_attn: float32 [4096], replicated
- w_q: bfloat16 [4096, 4096], P(None, 'tp')
- w_k: bfloat16 [4096, 1024], P(None, 'tp')
- w_v: bfloat16 [4096, 1024], P(None, 'tp')
- w_o: bfloat16 [4096, 4096], P('tp')
- gain_mlp: float32 [4096], replicated
- w_gate: bfloat16 [4096, 14336], P(None, 'tp')
- w_up: bfloat16 [4096, 14336], P(None, 'tp')
- w_down: bfloat16 [14336, 4096], P('tp')
Outputs:
- output 1: bfloat16 [8192, 4096], P(('rep', 'sp'))
- output 2: bfloat16 [8192, 32, 128], P('rep', ('tp', 'sp'))
- output 3: bfloat16 [8192, 32, 128], P('rep', ('tp', 'sp'))
All inputs are finite; a program needn't handle non-finite values.
Results may differ from the reference program's by a relative error of at most 0.00724617.
Values are sent between devices in bfloat16 or wider.
A program may use at most 768 MiB of HBM per device.

```python
import jax
import jax.numpy as jnp
from jax import lax

TOKENS = 8192
MODEL_DIM = 4096
FF_DIM = 14336
Q_HEADS = 32
KV_HEADS = 8
HEAD_DIM = 128
NUM_REQS = 2
KV_SLOTS = 32
ROPE_BASE = 500000
NORM_EPS = 1e-5


def draw_layout(layout_key):
    cut_key, step_key, start_key = jax.random.split(layout_key, 3)
    cut_rows = jnp.sort(jax.random.choice(cut_key, TOKENS - 1, (NUM_REQS - 1,), replace=False) + 1).astype(jnp.int32)
    tok_index = jnp.arange(TOKENS, dtype=jnp.int32)
    segments = jnp.sum(tok_index[:, None] >= cut_rows[None, :], axis=1).astype(jnp.int32)
    step_sizes = jax.random.randint(step_key, (TOKENS,), 1, 4, dtype=jnp.int32)
    run_sum = jnp.cumsum(step_sizes)
    first_rows = jnp.concatenate([jnp.zeros((1,), jnp.int32), cut_rows])
    seg_base = run_sum[first_rows] - step_sizes[first_rows]
    start_pos = jax.random.randint(start_key, (NUM_REQS,), 0, 1024, dtype=jnp.int32)
    positions = (run_sum - seg_base[segments] + start_pos[segments]).astype(jnp.int32)
    return positions, segments


def setup_inputs(seed: int = 0, part: int = 0) -> dict:
    base_key = jax.random.key(seed)
    part_key = jax.random.fold_in(base_key, part)
    x_key, layout_key = jax.random.split(part_key, 2)
    w_keys = jax.random.split(base_key, 10)
    positions, segments = draw_layout(layout_key)
    d_scale = MODEL_DIM ** -0.5

    def normal_weight(key_w, shape, std_dev):
        return (jax.random.normal(key_w, shape, jnp.float32) * std_dev).astype(jnp.bfloat16)

    return {
        "x_in": jax.random.normal(x_key, (TOKENS, MODEL_DIM), jnp.float32).astype(jnp.bfloat16),
        "positions": positions,
        "segments": segments,
        "gain_attn": 1.0 + 0.25 * jax.random.normal(w_keys[0], (MODEL_DIM,), jnp.float32),
        "w_q": normal_weight(w_keys[1], (MODEL_DIM, Q_HEADS * HEAD_DIM), 1.6 * d_scale),
        "w_k": normal_weight(w_keys[2], (MODEL_DIM, KV_HEADS * HEAD_DIM), 1.6 * d_scale),
        "w_v": normal_weight(w_keys[3], (MODEL_DIM, KV_HEADS * HEAD_DIM), d_scale),
        "w_o": normal_weight(w_keys[4], (Q_HEADS * HEAD_DIM, MODEL_DIM), (Q_HEADS * HEAD_DIM) ** -0.5),
        "gain_mlp": 1.0 + 0.25 * jax.random.normal(w_keys[5], (MODEL_DIM,), jnp.float32),
        "w_gate": normal_weight(w_keys[6], (MODEL_DIM, FF_DIM), d_scale),
        "w_up": normal_weight(w_keys[7], (MODEL_DIM, FF_DIM), d_scale),
        "w_down": normal_weight(w_keys[8], (FF_DIM, MODEL_DIM), FF_DIM ** -0.5),
    }


def rms_norm(x_f32, gain_vec):
    mean_sq = jnp.mean(x_f32 * x_f32, axis=-1, keepdims=True)
    return (x_f32 * lax.rsqrt(mean_sq + NORM_EPS) * gain_vec).astype(jnp.bfloat16)


def rope_tables(positions):
    half_dim = HEAD_DIM // 2
    inv_freq = jnp.power(jnp.float32(ROPE_BASE), -jnp.arange(half_dim, dtype=jnp.float32) * (2.0 / HEAD_DIM))
    angles = positions.astype(jnp.float32)[:, None] * inv_freq[None, :]
    return jnp.cos(angles)[:, None, :], jnp.sin(angles)[:, None, :]


def rotate(t_f32, cos_t, sin_t):
    half_dim = HEAD_DIM // 2
    t_lo = t_f32[..., :half_dim]
    t_hi = t_f32[..., half_dim:]
    return jnp.concatenate([t_lo * cos_t - t_hi * sin_t, t_hi * cos_t + t_lo * sin_t], axis=-1)


def reference(x_in, positions, segments, gain_attn, w_q, w_k, w_v, w_o, gain_mlp, w_gate, w_up, w_down):
    x_f32 = x_in.astype(jnp.float32)
    u_norm = rms_norm(x_f32, gain_attn)
    cos_t, sin_t = rope_tables(positions)
    q_rot = rotate(jnp.dot(u_norm, w_q, preferred_element_type=jnp.float32).reshape(TOKENS, Q_HEADS, HEAD_DIM), cos_t, sin_t).astype(jnp.bfloat16)
    k_rot = rotate(jnp.dot(u_norm, w_k, preferred_element_type=jnp.float32).reshape(TOKENS, KV_HEADS, HEAD_DIM), cos_t, sin_t).astype(jnp.bfloat16)
    v_proj = jnp.dot(u_norm, w_v, preferred_element_type=jnp.float32).astype(jnp.bfloat16).reshape(TOKENS, KV_HEADS, HEAD_DIM)
    group_size = Q_HEADS // KV_HEADS
    tok_index = jnp.arange(TOKENS)
    allowed = (tok_index[:, None] >= tok_index[None, :]) & (segments[:, None] == segments[None, :])
    score_scale = HEAD_DIM ** -0.5

    def one_head(operands):
        q_one, k_one, v_one = operands
        scores = jnp.dot(q_one, k_one.T, preferred_element_type=jnp.float32) * score_scale
        scores = jnp.where(allowed, scores, -1e30)
        prob_bf16 = jax.nn.softmax(scores, axis=-1).astype(jnp.bfloat16)
        return jnp.dot(prob_bf16, v_one, preferred_element_type=jnp.float32).astype(jnp.bfloat16)

    q_heads = jnp.transpose(q_rot, (1, 0, 2))
    k_heads = jnp.repeat(jnp.transpose(k_rot, (1, 0, 2)), group_size, axis=0)
    v_heads = jnp.repeat(jnp.transpose(v_proj, (1, 0, 2)), group_size, axis=0)
    attn_out = jnp.transpose(lax.map(one_head, (q_heads, k_heads, v_heads)), (1, 0, 2)).reshape(TOKENS, Q_HEADS * HEAD_DIM)
    x_mid = x_f32 + jnp.dot(attn_out, w_o, preferred_element_type=jnp.float32)
    u_mlp = rms_norm(x_mid, gain_mlp)
    gate_act = jnp.dot(u_mlp, w_gate, preferred_element_type=jnp.float32)
    up_act = jnp.dot(u_mlp, w_up, preferred_element_type=jnp.float32)
    hidden = (jax.nn.silu(gate_act) * up_act).astype(jnp.bfloat16)
    y_out = (x_mid + jnp.dot(hidden, w_down, preferred_element_type=jnp.float32)).astype(jnp.bfloat16)
    slot_repeat = KV_SLOTS // KV_HEADS
    return y_out, jnp.repeat(k_rot, slot_repeat, axis=1), jnp.repeat(v_proj, slot_repeat, axis=1)
```

```python
import functools
import math

import jax
import jax.numpy as jnp
from jax import lax
from jax.experimental import pallas as pl
from jax.experimental.pallas import tpu as pltpu
from jax.sharding import PartitionSpec as P

HEAD_DIM = 128
ROPE_BASE = 500000.0
NORM_EPS = 1e-5
NUM_REQS = 2
CHUNKS = 4
KV_BLOCK = 512
FF_TILE = 512
OUT_TILE = 256
SCORE_SCALE = HEAD_DIM ** -0.5 * math.log2(math.e)
MASKED = -1e30
F32 = jnp.float32
BF16 = jnp.bfloat16


def rms_norm(x_f32, gain_vec):
    mean_sq = jnp.mean(x_f32 * x_f32, axis=-1, keepdims=True)
    return (x_f32 * lax.rsqrt(mean_sq + NORM_EPS) * gain_vec).astype(BF16)


def rope_tables(positions):
    half_dim = HEAD_DIM // 2
    inv_freq = jnp.power(F32(ROPE_BASE), -jnp.arange(half_dim, dtype=F32) * (2.0 / HEAD_DIM))
    angles = positions.astype(F32)[..., None] * inv_freq
    return jnp.cos(angles)[..., None, :], jnp.sin(angles)[..., None, :]


def rotate(t_f32, cos_t, sin_t):
    half_dim = HEAD_DIM // 2
    t_lo = t_f32[..., :half_dim]
    t_hi = t_f32[..., half_dim:]
    return jnp.concatenate([t_lo * cos_t - t_hi * sin_t, t_hi * cos_t + t_lo * sin_t], axis=-1)


def attn_kernel(group, bounds_ref, q_ref, k_ref, v_ref, first_ref, after_ref, o_ref, m_scr, l_scr, acc_scr):
    rows = q_ref.shape[0]
    block = min(KV_BLOCK, k_ref.shape[0])
    lanes = block // HEAD_DIM
    row0, first_lo, first_hi = bounds_ref[0], bounds_ref[1], bounds_ref[2]
    m_scr[...] = jnp.full_like(m_scr, MASKED)
    l_scr[...] = jnp.zeros_like(l_scr)
    acc_scr[...] = jnp.zeros_like(acc_scr)

    start = lax.div(first_lo, block)
    stop = lax.div(row0 + (rows + block - 1), block)
    plain0 = jnp.minimum(lax.div(first_hi + (block - 1), block), stop)
    plain1 = jnp.maximum(lax.div(row0 + 1, block), plain0)
    n_low = plain0 - start

    def scores(head, key_rows):
        q_one = q_ref[:, head * HEAD_DIM:(head + 1) * HEAD_DIM]
        return lax.dot_general(q_one, key_rows, (((1,), (1,)), ((), ())), preferred_element_type=F32)

    def step(j, masked):
        offset = pl.multiple_of(j * block, block)
        key_rows = k_ref[pl.ds(offset, block), :]
        val_rows = v_ref[pl.ds(offset, block), :]
        if masked:
            k_index = offset + lax.broadcasted_iota(jnp.int32, (rows, block), 1)
            q_index = row0 + lax.broadcasted_iota(jnp.int32, (rows, block), 0)
            allowed = (k_index <= q_index) & (k_index >= first_ref[...])
        raw = scores(0, key_rows)
        for head in range(group):
            s = raw * SCORE_SCALE
            if head + 1 < group:
                raw = scores(head + 1, key_rows)
            if masked:
                s = jnp.where(allowed, s, MASKED)
            m_old = m_scr[head]
            m_new = jnp.maximum(m_old, jnp.max(s, axis=1, keepdims=True))
            alpha = jnp.exp2(m_old - m_new)
            p = jnp.exp2(s - jnp.concatenate([m_new] * lanes, axis=1))
            part = p[:, :HEAD_DIM]
            for i in range(1, lanes):
                part = part + p[:, i * HEAD_DIM:(i + 1) * HEAD_DIM]
            m_scr[head] = m_new
            l_scr[head] = alpha * l_scr[head] + part
            acc_scr[head] = alpha * acc_scr[head] + jnp.dot(p.astype(BF16), val_rows, preferred_element_type=F32)

    def plain_step(j, carry):
        step(j, False)
        return carry

    def masked_step(i, carry):
        step(jnp.where(i < n_low, start + i, plain1 + i - n_low), True)
        return carry

    lax.fori_loop(plain0, plain1, plain_step, 0)
    lax.fori_loop(0, n_low + stop - plain1, masked_step, 0)
    for head in range(group):
        total = jnp.sum(l_scr[head], axis=1, keepdims=True)
        o_ref[:, head * HEAD_DIM:(head + 1) * HEAD_DIM] = (acc_scr[head] / total).astype(BF16)


def attention_chunk(bounds, q_rot, kv_all, first_rows, chunk, rows, kv_local, after):
    tokens = kv_all.shape[0]
    width = q_rot.shape[1] // kv_local
    group = width // HEAD_DIM
    flops = 4 * rows * q_rot.shape[1] * tokens // 2
    return pl.pallas_call(
        functools.partial(attn_kernel, group),
        out_shape=jax.ShapeDtypeStruct((rows, q_rot.shape[1]), BF16),
        grid_spec=pltpu.PrefetchScalarGridSpec(
            num_scalar_prefetch=1,
            grid=(kv_local,),
            in_specs=[
                pl.BlockSpec((rows, width), lambda g, b: (chunk, g)),
                pl.BlockSpec((tokens, HEAD_DIM), lambda g, b: (0, g)),
                pl.BlockSpec((tokens, HEAD_DIM), lambda g, b: (0, kv_local + g)),
                pl.BlockSpec((rows, 1), lambda g, b: (chunk, 0)),
                pl.BlockSpec(memory_space=pl.ANY),
            ],
            out_specs=pl.BlockSpec((rows, width), lambda g, b: (0, g)),
            scratch_shapes=[pltpu.VMEM((group, rows, HEAD_DIM), F32)] * 3,
        ),
        compiler_params=pltpu.CompilerParams(dimension_semantics=("arbitrary",), vmem_limit_bytes=40 * 2 ** 20),
        cost_estimate=pl.CostEstimate(flops=3 * flops, bytes_accessed=2 * kv_all.size, transcendentals=flops // 256),
        name=f"attn{chunk}",
    )(bounds, q_rot, kv_all, kv_all, first_rows, after)


def out_proj_kernel(a_ref, w_ref, x_ref, after_ref, o_ref, ssq_ref):
    parts, slabs = a_ref.shape[0], w_ref.shape[0]
    total = x_ref[...].astype(F32)
    acc = None
    for j in range(parts):
        w_cols = jnp.concatenate([w_ref[s, j] for s in range(slabs)], axis=0)
        term = jnp.dot(a_ref[j], w_cols, preferred_element_type=F32)
        acc = term if acc is None else acc + term
    total = total + acc
    o_ref[...] = total
    squares = total * total
    part = squares[:, :128]
    for i in range(1, squares.shape[1] // 128):
        part = part + squares[:, i * 128:(i + 1) * 128]

    @pl.when(pl.program_id(0) == 0)
    def _():
        ssq_ref[...] = part

    @pl.when(pl.program_id(0) > 0)
    def _():
        ssq_ref[...] += part


def out_proj(attn_all, wo_cols, x_cols, chunk, after):
    parts, rows, depth = attn_all.shape
    slabs, _, slab_rows, cols = wo_cols.shape
    tile = min(OUT_TILE, cols)
    return pl.pallas_call(
        out_proj_kernel,
        out_shape=(jax.ShapeDtypeStruct((rows, cols), F32), jax.ShapeDtypeStruct((rows, 128), F32)),
        grid=(cols // tile,),
        in_specs=[
            pl.BlockSpec((parts, rows, depth), lambda n: (0, 0, 0)),
            pl.BlockSpec((slabs, parts, slab_rows, tile), lambda n: (0, 0, 0, n)),
            pl.BlockSpec((rows, tile), lambda n: (chunk, n)),
            pl.BlockSpec(memory_space=pl.ANY),
        ],
        out_specs=(pl.BlockSpec((rows, tile), lambda n: (0, n)), pl.BlockSpec((rows, 128), lambda n: (0, 0))),
        compiler_params=pltpu.CompilerParams(dimension_semantics=("arbitrary",), vmem_limit_bytes=40 * 2 ** 20),
        cost_estimate=pl.CostEstimate(flops=2 * rows * parts * depth * cols, bytes_accessed=2 * wo_cols.size, transcendentals=0),
        name=f"outproj{chunk}",
    )(attn_all, wo_cols, x_cols, after)


def mlp_kernel(u_ref, wg_ref, wu_ref, wd_ref, after_ref, o_ref):
    parts, rows, depth = u_ref.shape
    cols = o_ref.shape[2]

    def project(w_ref):
        acc = None
        for j in range(parts):
            term = jnp.dot(u_ref[j], w_ref[j * depth:(j + 1) * depth, :], preferred_element_type=F32)
            acc = term if acc is None else acc + term
        return acc

    hidden = (jax.nn.silu(project(wg_ref)) * project(wu_ref)).astype(BF16)

    @pl.when(pl.program_id(0) == 0)
    def _():
        for j in range(o_ref.shape[0]):
            o_ref[j] = jnp.dot(hidden, wd_ref[:, j * cols:(j + 1) * cols], preferred_element_type=F32)

    @pl.when(pl.program_id(0) > 0)
    def _():
        for j in range(o_ref.shape[0]):
            o_ref[j] += jnp.dot(hidden, wd_ref[:, j * cols:(j + 1) * cols], preferred_element_type=F32)


def mlp_partial(u_all, w_gate, w_up, w_down, chunk, after):
    parts, rows, depth = u_all.shape
    ff_local = w_gate.shape[1]
    tile = FF_TILE
    model = w_down.shape[1]
    return pl.pallas_call(
        mlp_kernel,
        out_shape=jax.ShapeDtypeStruct((parts, rows, model // parts), F32),
        grid=(ff_local // tile,),
        in_specs=[
            pl.BlockSpec((parts, rows, depth), lambda i: (0, 0, 0)),
            pl.BlockSpec((parts * depth, tile), lambda i: (0, i)),
            pl.BlockSpec((parts * depth, tile), lambda i: (0, i)),
            pl.BlockSpec((tile, model), lambda i: (i, 0)),
            pl.BlockSpec(memory_space=pl.ANY),
        ],
        out_specs=pl.BlockSpec((parts, rows, model // parts), lambda i: (0, 0, 0)),
        compiler_params=pltpu.CompilerParams(dimension_semantics=("arbitrary",), vmem_limit_bytes=56 * 2 ** 20),
        cost_estimate=pl.CostEstimate(flops=6 * rows * model * ff_local, bytes_accessed=6 * model * ff_local,
                                      transcendentals=rows * ff_local),
        name=f"mlp{chunk}",
    )(u_all, w_gate, w_up, w_down, after)


def pipeline_order(chunks):
    order = []
    for tick in range(chunks + 3):
        if tick < chunks:
            order.append(("attn", tick))
        if 1 <= tick <= chunks:
            order.append(("out", tick - 1))
        if 3 <= tick:
            order.append(("mlp", tick - 3))
    return order


def solution(mesh):
    sp_size = mesh.shape["sp"]
    tp_size = mesh.shape["tp"]
    row_spec = P(("rep", "sp"), None)
    tok_spec = P(("rep", "sp"))
    full_spec = P(None)
    col_spec = P(None, "tp")
    wrow_spec = P("tp", None)
    cache_spec = P("rep", ("tp", "sp"), None)

    def local_layer(x_in, positions, segments, gain_attn, w_q, w_k, w_v, w_o, gain_mlp, w_gate, w_up, w_down):
        rows_local, model = x_in.shape
        kv_local = w_k.shape[1] // HEAD_DIM
        heads_local = w_q.shape[1] // HEAD_DIM
        kv_repeat = sp_size // kv_local
        rows = rows_local // CHUNKS
        cols = model // tp_size
        sp_rank = lax.axis_index("sp")
        tp_rank = lax.axis_index("tp")
        row_base = sp_rank * rows_local

        below = jnp.sum(segments[:, None] < jnp.arange(NUM_REQS)[None, :], axis=0, dtype=jnp.int32)
        starts = lax.psum(below, "sp")
        first_rows = jnp.sum(jnp.where(segments[:, None] == jnp.arange(NUM_REQS)[None, :], starts[None, :], 0), axis=1,
                             dtype=jnp.int32)

        x_f32 = x_in.astype(F32)
        u_norm = rms_norm(x_f32, gain_attn)
        cos_t, sin_t = rope_tables(positions)
        k_rot = rotate(jnp.dot(u_norm, w_k, preferred_element_type=F32).reshape(rows_local, -1, HEAD_DIM), cos_t, sin_t).astype(BF16)
        v_proj = jnp.dot(u_norm, w_v, preferred_element_type=F32).astype(BF16)
        kv_own = jnp.concatenate([k_rot.reshape(rows_local, -1), v_proj], axis=1)
        kv_all = lax.all_gather(kv_own, "sp", tiled=True)
        q_rot = rotate(jnp.dot(u_norm, w_q, preferred_element_type=F32).reshape(rows_local, -1, HEAD_DIM), cos_t, sin_t).astype(BF16)
        q_rot = q_rot.reshape(rows_local, -1)
        slot_head = sp_rank // kv_repeat
        k_cache = lax.dynamic_slice_in_dim(kv_all, slot_head * HEAD_DIM, HEAD_DIM, axis=1)[:, None, :]
        v_cache = lax.dynamic_slice_in_dim(kv_all, (kv_local + slot_head) * HEAD_DIM, HEAD_DIM, axis=1)[:, None, :]

        slab_rows = heads_local * HEAD_DIM // sp_size
        slab = lax.dynamic_slice_in_dim(w_o, sp_rank * slab_rows, slab_rows, axis=0)
        slab = jnp.transpose(slab.reshape(slab_rows, tp_size, cols), (1, 0, 2))
        slab = lax.all_to_all(slab, "tp", 0, 0, tiled=True)
        wo_cols = lax.all_gather(slab, "sp")
        x_cols = lax.dynamic_slice_in_dim(x_in, tp_rank * cols, cols, axis=1)
        gain_cols = lax.dynamic_slice_in_dim(gain_mlp, tp_rank * cols, cols, axis=0)

        attn_all, x_mid, u_all, y_parts = {}, {}, {}, {}
        after = q_rot
        for stage, chunk in pipeline_order(CHUNKS):
            row0 = chunk * rows
            if stage == "attn":
                bounds = jnp.stack([row_base + row0, first_rows[row0], first_rows[row0 + rows - 1]])
                after = attention_chunk(bounds, q_rot, kv_all, first_rows[:, None], chunk, rows, kv_local, after)
                attn_all[chunk] = lax.all_gather(after, "tp")
            elif stage == "out":
                x_mid[chunk], ssq = out_proj(attn_all[chunk], wo_cols, x_cols, chunk, after)
                sum_sq = lax.psum(jnp.sum(ssq, axis=1), "tp")
                u_own = (x_mid[chunk] * lax.rsqrt(sum_sq[:, None] / model + NORM_EPS) * gain_cols).astype(BF16)
                u_all[chunk] = lax.all_gather(u_own, "tp")
                after = u_own
            else:
                after = mlp_partial(u_all[chunk], w_gate, w_up, w_down, chunk, after)
                down = lax.psum_scatter(after, "tp", scatter_dimension=0, tiled=False)
                y_parts[chunk] = lax.all_gather((x_mid[chunk] + down).astype(BF16), "tp")
        pieces = [jnp.transpose(y_parts[chunk], (1, 0, 2)).reshape(rows, model) for chunk in range(CHUNKS)]
        y_out = jnp.concatenate(pieces, axis=0)
        return y_out, k_cache, v_cache

    return jax.shard_map(local_layer, mesh=mesh,
                         in_specs=(row_spec, tok_spec, tok_spec, full_spec, col_spec, col_spec, col_spec, wrow_spec,
                                   full_spec, col_spec, col_spec, wrow_spec),
                         out_specs=(row_spec, cache_spec, cache_spec), check_vma=False)
```

```python
import functools
import math

import jax
import jax.numpy as jnp
from jax import lax
from jax.experimental import pallas as pl
from jax.experimental.pallas import tpu as pltpu
from jax.sharding import PartitionSpec as P


HEAD_DIM = 128
ROPE_BASE = 500000.0
NORM_EPS = 1e-5
NUM_REQS = 2
CHUNKS = 4
KV_BLOCK = 512
FF_TILE = 512
OUT_TILE = 256
VMEM_GRANT = 63_000_000
SCORE_SCALE = HEAD_DIM ** -0.5 * math.log2(math.e)
MASKED = -1e30
F32 = jnp.float32
BF16 = jnp.bfloat16


def rms_norm(x_f32, gain_vec):
    mean_sq = jnp.mean(x_f32 * x_f32, axis=-1, keepdims=True)
    return (x_f32 * lax.rsqrt(mean_sq + NORM_EPS) * gain_vec).astype(BF16)


def rope_tables(positions):
    half_dim = HEAD_DIM // 2
    inv_freq = jnp.power(F32(ROPE_BASE), -jnp.arange(half_dim, dtype=F32) * (2.0 / HEAD_DIM))
    angles = positions.astype(F32)[..., None] * inv_freq
    return jnp.cos(angles)[..., None, :], jnp.sin(angles)[..., None, :]


def rotate(t_f32, cos_t, sin_t):
    half_dim = HEAD_DIM // 2
    t_lo = t_f32[..., :half_dim]
    t_hi = t_f32[..., half_dim:]
    return jnp.concatenate([t_lo * cos_t - t_hi * sin_t, t_hi * cos_t + t_lo * sin_t], axis=-1)


def attn_kernel(group, bounds_ref, q_ref, k_ref, v_ref, first_ref, *refs):
    o_ref, q_scr, m_scr, l_scr, acc_scr = refs[-5:]
    rows = q_ref.shape[0]
    block = min(KV_BLOCK, k_ref.shape[0])
    row0, first_lo, first_hi = bounds_ref[0], bounds_ref[1], bounds_ref[2]
    m_scr[...] = jnp.full_like(m_scr, MASKED)
    l_scr[...] = jnp.zeros_like(l_scr)
    acc_scr[...] = jnp.zeros_like(acc_scr)
    for head in range(group):
        q_one = q_ref[:, head * HEAD_DIM:(head + 1) * HEAD_DIM]
        q_scr[head] = jnp.transpose(q_one.astype(F32)).astype(BF16)

    start = lax.div(first_lo, block)
    stop = lax.div(row0 + (rows + block - 1), block)
    plain0 = jnp.minimum(lax.div(first_hi + (block - 1), block), stop)
    plain1 = jnp.maximum(lax.div(row0 + 1, block), plain0)
    n_low = plain0 - start

    def step(j, masked):
        offset = pl.multiple_of(j * block, block)
        key_rows = k_ref[pl.ds(offset, block), :]
        val_cols = jnp.transpose(v_ref[pl.ds(offset, block), :])
        if masked:
            k_index = offset + lax.broadcasted_iota(jnp.int32, (block, rows), 0)
            q_index = row0 + lax.broadcasted_iota(jnp.int32, (block, rows), 1)
            allowed = (k_index <= q_index) & (k_index >= first_ref[...])
        raw = jnp.dot(key_rows, q_scr[0], preferred_element_type=F32)
        for head in range(group):
            s = raw * SCORE_SCALE
            if head + 1 < group:
                raw = jnp.dot(key_rows, q_scr[head + 1], preferred_element_type=F32)
            if masked:
                s = jnp.where(allowed, s, MASKED)
            m_old = m_scr[head]
            m_new = jnp.maximum(m_old, jnp.max(s, axis=0, keepdims=True))
            alpha = jnp.exp2(m_old - m_new)
            p = jnp.exp2(s - m_new)
            m_scr[head] = m_new
            l_scr[head] = alpha * l_scr[head] + jnp.sum(p.reshape(block // 8, 8, rows), axis=0)
            acc_scr[head] = alpha * acc_scr[head] + jnp.dot(val_cols, p.astype(BF16), preferred_element_type=F32)

    def plain_step(j, carry):
        step(j, False)
        return carry

    def masked_step(i, carry):
        step(jnp.where(i < n_low, start + i, plain1 + i - n_low), True)
        return carry

    lax.fori_loop(plain0, plain1, plain_step, 0)
    lax.fori_loop(0, n_low + stop - plain1, masked_step, 0)
    for head in range(group):
        total = jnp.sum(l_scr[head], axis=0, keepdims=True)
        o_ref[:, head * HEAD_DIM:(head + 1) * HEAD_DIM] = jnp.transpose(acc_scr[head] / total).astype(BF16)


def attention_chunk(bounds, q_rot, kv_all, first_rows, chunk, rows, kv_local, after):
    tokens = kv_all.shape[0]
    width = q_rot.shape[1] // kv_local
    group = width // HEAD_DIM
    flops = 4 * rows * q_rot.shape[1] * tokens
    return pl.pallas_call(
        functools.partial(attn_kernel, group),
        out_shape=jax.ShapeDtypeStruct((rows, q_rot.shape[1]), BF16),
        grid_spec=pltpu.PrefetchScalarGridSpec(
            num_scalar_prefetch=1,
            grid=(kv_local,),
            in_specs=[
                pl.BlockSpec((rows, width), lambda g, b: (chunk, g)),
                pl.BlockSpec((tokens, HEAD_DIM), lambda g, b: (0, g)),
                pl.BlockSpec((tokens, HEAD_DIM), lambda g, b: (0, kv_local + g)),
                pl.BlockSpec((1, rows), lambda g, b: (0, chunk)),
            ] + [pl.BlockSpec(memory_space=pl.ANY)] * len(after),
            out_specs=pl.BlockSpec((rows, width), lambda g, b: (0, g)),
            scratch_shapes=[
                pltpu.VMEM((group, HEAD_DIM, rows), BF16),
                pltpu.VMEM((group, 1, rows), F32),
                pltpu.VMEM((group, 8, rows), F32),
                pltpu.VMEM((group, HEAD_DIM, rows), F32),
            ],
        ),
        compiler_params=pltpu.CompilerParams(dimension_semantics=("arbitrary",), vmem_limit_bytes=VMEM_GRANT),
        cost_estimate=pl.CostEstimate(flops=2 * flops, bytes_accessed=2 * kv_all.size, transcendentals=flops // 512),
    )(bounds, q_rot, kv_all, kv_all, first_rows, *after)


def out_proj_kernel(parts, *refs):
    a_refs, (w_ref, x_ref), (o_ref, ssq_ref) = refs[:parts], refs[parts:parts + 2], refs[-2:]
    slabs = w_ref.shape[0]
    acc = None
    for j in range(parts):
        w_cols = jnp.concatenate([w_ref[s, j] for s in range(slabs)], axis=0)
        term = jnp.dot(a_refs[j][...], w_cols, preferred_element_type=F32)
        acc = term if acc is None else acc + term
    total = x_ref[...].astype(F32) + acc
    o_ref[...] = total
    squares = total * total
    part = squares[:, :128]
    for i in range(1, squares.shape[1] // 128):
        part = part + squares[:, i * 128:(i + 1) * 128]

    @pl.when(pl.program_id(0) == 0)
    def _():
        ssq_ref[...] = part

    @pl.when(pl.program_id(0) > 0)
    def _():
        ssq_ref[...] += part


def out_proj(attn_parts, wo_cols, x_cols, chunk, after):
    parts = len(attn_parts)
    rows, depth = attn_parts[0].shape
    slabs, _, slab_rows, cols = wo_cols.shape
    tile = min(OUT_TILE, cols)
    return pl.pallas_call(
        functools.partial(out_proj_kernel, parts),
        out_shape=(jax.ShapeDtypeStruct((rows, cols), F32), jax.ShapeDtypeStruct((rows, 128), F32)),
        grid=(cols // tile,),
        in_specs=[pl.BlockSpec((rows, depth), lambda n: (0, 0))] * parts + [
            pl.BlockSpec((slabs, parts, slab_rows, tile), lambda n: (0, 0, 0, n)),
            pl.BlockSpec((rows, tile), lambda n: (chunk, n)),
        ] + [pl.BlockSpec(memory_space=pl.ANY)] * len(after),
        out_specs=(pl.BlockSpec((rows, tile), lambda n: (0, n)), pl.BlockSpec((rows, 128), lambda n: (0, 0))),
        compiler_params=pltpu.CompilerParams(dimension_semantics=("arbitrary",), vmem_limit_bytes=VMEM_GRANT),
        cost_estimate=pl.CostEstimate(flops=2 * rows * parts * depth * cols, bytes_accessed=2 * wo_cols.size, transcendentals=0),
    )(*attn_parts, wo_cols, x_cols, *after)


def mlp_kernel(parts, rank_ref, *refs):
    u_refs, (wg_ref, wu_ref, wd_ref), o_ref = refs[:parts], refs[parts:parts + 3], refs[-1]
    depth = u_refs[0].shape[1]
    cols = o_ref.shape[2]

    def project(w_ref):
        acc = None
        for j in range(parts):
            owner = lax.rem(rank_ref[0] + j, parts)
            w_rows = w_ref[pl.ds(pl.multiple_of(owner * depth, depth), depth), :]
            term = jnp.dot(u_refs[j][...], w_rows, preferred_element_type=F32)
            acc = term if acc is None else acc + term
        return acc

    hidden = (jax.nn.silu(project(wg_ref)) * project(wu_ref)).astype(BF16)

    @pl.when(pl.program_id(0) == 0)
    def _():
        for j in range(o_ref.shape[0]):
            o_ref[j] = jnp.dot(hidden, wd_ref[:, j * cols:(j + 1) * cols], preferred_element_type=F32)

    @pl.when(pl.program_id(0) > 0)
    def _():
        for j in range(o_ref.shape[0]):
            o_ref[j] += jnp.dot(hidden, wd_ref[:, j * cols:(j + 1) * cols], preferred_element_type=F32)


def mlp_partial(rank, u_parts, w_gate, w_up, w_down, after):
    if isinstance(u_parts, list):
        parts = len(u_parts)
        rows, depth = u_parts[0].shape
        u_specs = [pl.BlockSpec((rows, depth), lambda i, r: (0, 0))] * parts
    else:
        parts, rows, depth = u_parts.shape
        u_specs = [pl.BlockSpec((None, rows, depth), lambda i, r, j=j: (j, 0, 0)) for j in range(parts)]
        u_parts = [u_parts] * parts
    ff_local = w_gate.shape[1]
    tile = FF_TILE
    model = w_down.shape[1]
    return pl.pallas_call(
        functools.partial(mlp_kernel, parts),
        out_shape=jax.ShapeDtypeStruct((parts, rows, model // parts), F32),
        grid_spec=pltpu.PrefetchScalarGridSpec(
            num_scalar_prefetch=1,
            grid=(ff_local // tile,),
            in_specs=u_specs + [
                pl.BlockSpec((parts * depth, tile), lambda i, r: (0, i)),
                pl.BlockSpec((parts * depth, tile), lambda i, r: (0, i)),
                pl.BlockSpec((tile, model), lambda i, r: (i, 0)),
            ] + [pl.BlockSpec(memory_space=pl.ANY)] * len(after),
            out_specs=pl.BlockSpec((parts, rows, model // parts), lambda i, r: (0, 0, 0)),
        ),
        compiler_params=pltpu.CompilerParams(dimension_semantics=("arbitrary",), vmem_limit_bytes=VMEM_GRANT),
        cost_estimate=pl.CostEstimate(flops=6 * rows * model * ff_local, bytes_accessed=6 * model * ff_local,
                                      transcendentals=rows * ff_local),
    )(rank, *u_parts, w_gate, w_up, w_down, *after)


def join_kernel(parts, rank_ref, *refs):
    part_refs, o_ref = refs[:parts], refs[-1]
    cols = part_refs[0].shape[1]
    for j in range(parts):
        owner = lax.rem(rank_ref[0] + j, parts)
        o_ref[:, pl.ds(pl.multiple_of(owner * cols, cols), cols)] = part_refs[j][...]


def join(rank, y_parts, y_out, chunk, chunks):
    parts = len(y_parts)
    rows, cols = y_parts[0].shape
    in_specs = [pl.BlockSpec((rows, cols), lambda i, r: (0, 0))] * parts
    operands = [rank, *y_parts]
    aliases = {}
    if y_out is not None:
        aliases = {len(operands): 0}
        in_specs = in_specs + [pl.BlockSpec(memory_space=pl.ANY)]
        operands.append(y_out)
    return pl.pallas_call(
        functools.partial(join_kernel, parts),
        out_shape=jax.ShapeDtypeStruct((rows * chunks, parts * cols), BF16),
        grid_spec=pltpu.PrefetchScalarGridSpec(
            num_scalar_prefetch=1,
            grid=(1,),
            in_specs=in_specs,
            out_specs=pl.BlockSpec((rows, parts * cols), lambda i, r: (chunk, 0)),
        ),
        input_output_aliases=aliases,
        compiler_params=pltpu.CompilerParams(dimension_semantics=("arbitrary",), vmem_limit_bytes=VMEM_GRANT),
        cost_estimate=pl.CostEstimate(flops=0, bytes_accessed=4 * rows * parts * cols, transcendentals=0),
    )(*operands)


def ring_gather(own, axis, size, forward):
    def shifted(block, shift):
        return lax.ppermute(block, axis, [(i, (i + shift) % size) for i in range(size)])

    if size != 4:
        return [own] + [shifted(own, -k) for k in range(1, size)]
    before = shifted(own, 1)
    behind = shifted(own, -1)
    opposite = shifted(before, 1) if forward else shifted(behind, -1)
    return [own, behind, opposite, before]


def pipeline_order(chunks):
    order = [("attn", 0), ("attn", 1)]
    for chunk in range(2, chunks):
        order += [("attn", chunk), ("out", chunk - 2)]
    order += [("out", chunks - 2), ("mlp", 0), ("out", chunks - 1)]
    return order + [("mlp", chunk) for chunk in range(1, chunks)]


def solution(mesh):
    sp_size = mesh.shape["sp"]
    tp_size = mesh.shape["tp"]
    row_spec = P(("rep", "sp"), None)
    tok_spec = P(("rep", "sp"))
    full_spec = P(None)
    col_spec = P(None, "tp")
    wrow_spec = P("tp", None)
    cache_spec = P("rep", ("tp", "sp"), None)

    def local_layer(x_in, positions, segments, gain_attn, w_q, w_k, w_v, w_o, gain_mlp, w_gate, w_up, w_down):
        rows_local, model = x_in.shape
        kv_local = w_k.shape[1] // HEAD_DIM
        heads_local = w_q.shape[1] // HEAD_DIM
        kv_repeat = sp_size // kv_local
        rows = rows_local // CHUNKS
        cols = model // tp_size
        sp_rank = lax.axis_index("sp")
        tp_rank = lax.axis_index("tp")
        row_base = sp_rank * rows_local

        below = jnp.sum(segments[:, None] < jnp.arange(NUM_REQS)[None, :], axis=0, dtype=jnp.int32)
        starts = lax.psum(below, "sp")
        first_rows = jnp.sum(jnp.where(segments[:, None] == jnp.arange(NUM_REQS)[None, :], starts[None, :], 0), axis=1,
                             dtype=jnp.int32)

        x_f32 = x_in.astype(F32)
        u_norm = rms_norm(x_f32, gain_attn)
        cos_t, sin_t = rope_tables(positions)
        k_rot = rotate(jnp.dot(u_norm, w_k, preferred_element_type=F32).reshape(rows_local, -1, HEAD_DIM), cos_t, sin_t).astype(BF16)
        v_proj = jnp.dot(u_norm, w_v, preferred_element_type=F32).astype(BF16)
        kv_own = jnp.concatenate([k_rot.reshape(rows_local, -1), v_proj], axis=1)
        kv_all = lax.all_gather(kv_own, "sp", tiled=True)
        q_rot = rotate(jnp.dot(u_norm, w_q, preferred_element_type=F32).reshape(rows_local, -1, HEAD_DIM), cos_t, sin_t).astype(BF16)
        q_rot = q_rot.reshape(rows_local, -1)
        slot_head = sp_rank // kv_repeat
        k_cache = lax.dynamic_slice_in_dim(kv_all, slot_head * HEAD_DIM, HEAD_DIM, axis=1)[:, None, :]
        v_cache = lax.dynamic_slice_in_dim(kv_all, (kv_local + slot_head) * HEAD_DIM, HEAD_DIM, axis=1)[:, None, :]

        slab_rows = heads_local * HEAD_DIM // sp_size
        slab = lax.dynamic_slice_in_dim(w_o, sp_rank * slab_rows, slab_rows, axis=0)
        slabs = [lax.dynamic_slice_in_dim(slab, tp_rank * cols, cols, axis=1)]
        for k in range(1, tp_size):
            block = lax.dynamic_slice_in_dim(slab, lax.rem(tp_rank + tp_size - k, tp_size) * cols, cols, axis=1)
            slabs.append(lax.ppermute(block, "tp", [(i, (i + tp_size - k) % tp_size) for i in range(tp_size)]))
        wo_cols = lax.all_gather(jnp.stack(slabs), "sp")
        x_cols = lax.dynamic_slice_in_dim(x_in, tp_rank * cols, cols, axis=1)
        gain_cols = lax.dynamic_slice_in_dim(gain_mlp, tp_rank * cols, cols, axis=0)

        rank = jnp.reshape(tp_rank, (1,)).astype(jnp.int32)
        rank_zero = jnp.zeros((1,), jnp.int32)
        attn_all, x_mid, u_all, y_own, y_all = {}, {}, {}, {}, {}
        after = [q_rot]
        for stage, chunk in pipeline_order(CHUNKS):
            row0 = chunk * rows
            forward = chunk % 2 == 0
            if stage == "attn":
                if chunk >= 2:
                    after = after + [attn_all[chunk - 2][1], attn_all[chunk - 2][-1]]
                bounds = jnp.stack([row_base + row0, first_rows[row0], first_rows[row0 + rows - 1]])
                attn_own = attention_chunk(bounds, q_rot, kv_all, first_rows[None, :], chunk, rows, kv_local, after)
                attn_all[chunk] = ring_gather(attn_own, "tp", tp_size, forward)
                after = [attn_own]
            elif stage == "out":
                if chunk == CHUNKS - 1 and CHUNKS >= 4 and tp_size == 4:
                    after = after + [u_all[2][1], u_all[2][-1]]
                x_mid[chunk], ssq = out_proj(attn_all[chunk], wo_cols, x_cols, chunk, after)
                sum_sq = lax.psum(jnp.sum(ssq, axis=1), "tp")
                u_own = (x_mid[chunk] * lax.rsqrt(sum_sq[:, None] / model + NORM_EPS) * gain_cols).astype(BF16)
                on_queue = chunk < 2
                u_all[chunk] = lax.all_gather(u_own, "tp") if on_queue else ring_gather(u_own, "tp", tp_size, forward)
                after = [u_own]
            else:
                if chunk >= 2:
                    after = after + [u_all[chunk][1], u_all[chunk][-1], y_own[chunk - 2]]
                if chunk + 1 < CHUNKS and isinstance(u_all[chunk + 1], list):
                    after = after + [u_all[chunk + 1][1], u_all[chunk + 1][-1]]
                if chunk >= 3:
                    after = after + [y_all[chunk - 3][1], y_all[chunk - 3][-1]]
                own_rank = rank if isinstance(u_all[chunk], list) else rank_zero
                if chunk == 0:
                    after = after + [attn_all[CHUNKS - 1][1], attn_all[CHUNKS - 1][-1]]
                partial = mlp_partial(own_rank, u_all[chunk], w_gate, w_up, w_down, after)
                down = lax.psum_scatter(partial, "tp", scatter_dimension=0, tiled=False)
                y_own[chunk] = (x_mid[chunk] + down).astype(BF16)
                y_all[chunk] = ring_gather(y_own[chunk], "tp", tp_size, forward)
                after = [partial]
        y_out = None
        for chunk in range(CHUNKS):
            y_out = join(rank, y_all[chunk], y_out, chunk, CHUNKS)
        return y_out, k_cache, v_cache

    return jax.shard_map(local_layer, mesh=mesh,
                         in_specs=(row_spec, tok_spec, tok_spec, full_spec, col_spec, col_spec, col_spec, wrow_spec,
                                   full_spec, col_spec, col_spec, wrow_spec),
                         out_specs=(row_spec, cache_spec, cache_spec), check_vma=False)
```

```python
import functools
import math

import jax
import jax.numpy as jnp
from jax import lax
from jax.experimental import pallas as pl
from jax.experimental.pallas import tpu as pltpu
from jax.sharding import PartitionSpec as P


HEAD_DIM = 128
ROPE_BASE = 500000.0
NORM_EPS = 1e-5
NUM_REQS = 2
CHUNKS = 4
KV_BLOCK = 512
FF_TILE = 512
OUT_TILE = 256
VMEM_GRANT = 63_000_000
SCORE_SCALE = HEAD_DIM ** -0.5 * math.log2(math.e)
MASKED = -1e30
F32 = jnp.float32
BF16 = jnp.bfloat16


def rms_norm(x_f32, gain_vec):
    mean_sq = jnp.mean(x_f32 * x_f32, axis=-1, keepdims=True)
    return (x_f32 * lax.rsqrt(mean_sq + NORM_EPS) * gain_vec).astype(BF16)


def rope_tables(positions):
    half_dim = HEAD_DIM // 2
    inv_freq = jnp.power(F32(ROPE_BASE), -jnp.arange(half_dim, dtype=F32) * (2.0 / HEAD_DIM))
    angles = positions.astype(F32)[..., None] * inv_freq
    return jnp.cos(angles)[..., None, :], jnp.sin(angles)[..., None, :]


def rotate(t_f32, cos_t, sin_t):
    half_dim = HEAD_DIM // 2
    t_lo = t_f32[..., :half_dim]
    t_hi = t_f32[..., half_dim:]
    return jnp.concatenate([t_lo * cos_t - t_hi * sin_t, t_hi * cos_t + t_lo * sin_t], axis=-1)


def attn_kernel(group, chunk, bounds_ref, q_ref, k_ref, v_ref, first_ref, *refs):
    o_ref, q_scr, m_scr, l_scr, acc_scr = refs[-5:]
    rows = q_ref.shape[0]
    block = min(KV_BLOCK, k_ref.shape[0])
    row0, first_lo, first_hi = bounds_ref[3 * chunk], bounds_ref[3 * chunk + 1], bounds_ref[3 * chunk + 2]
    m_scr[...] = jnp.full_like(m_scr, MASKED)
    l_scr[...] = jnp.zeros_like(l_scr)
    acc_scr[...] = jnp.zeros_like(acc_scr)
    for head in range(group):
        q_one = q_ref[:, head * HEAD_DIM:(head + 1) * HEAD_DIM]
        q_scr[head] = jnp.transpose(q_one.astype(F32)).astype(BF16)

    start = lax.div(first_lo, block)
    stop = lax.div(row0 + (rows + block - 1), block)
    plain0 = jnp.minimum(lax.div(first_hi + (block - 1), block), stop)
    plain1 = jnp.maximum(lax.div(row0 + 1, block), plain0)
    n_low = plain0 - start

    def step(j, masked):
        offset = pl.multiple_of(j * block, block)
        key_rows = k_ref[pl.ds(offset, block), :]
        val_cols = jnp.transpose(v_ref[pl.ds(offset, block), :])
        if masked:
            k_index = offset + lax.broadcasted_iota(jnp.int32, (block, rows), 0)
            q_index = row0 + lax.broadcasted_iota(jnp.int32, (block, rows), 1)
            allowed = (k_index <= q_index) & (k_index >= first_ref[...])
        raw = jnp.dot(key_rows, q_scr[0], preferred_element_type=F32)
        for head in range(group):
            s = raw * SCORE_SCALE
            if head + 1 < group:
                raw = jnp.dot(key_rows, q_scr[head + 1], preferred_element_type=F32)
            if masked:
                s = jnp.where(allowed, s, MASKED)
            m_old = m_scr[head]
            m_new = jnp.maximum(m_old, jnp.max(s, axis=0, keepdims=True))
            alpha = jnp.exp2(m_old - m_new)
            p = jnp.exp2(s - m_new)
            m_scr[head] = m_new
            l_scr[head] = alpha * l_scr[head] + jnp.sum(p.reshape(block // 8, 8, rows), axis=0)
            acc_scr[head] = alpha * acc_scr[head] + jnp.dot(val_cols, p.astype(BF16), preferred_element_type=F32)

    def plain_step(j, carry):
        step(j, False)
        return carry

    def masked_step(i, carry):
        step(jnp.where(i < n_low, start + i, plain1 + i - n_low), True)
        return carry

    lax.fori_loop(plain0, plain1, plain_step, 0)
    lax.fori_loop(0, n_low + stop - plain1, masked_step, 0)
    for head in range(group):
        total = jnp.sum(l_scr[head], axis=0, keepdims=True)
        o_ref[:, head * HEAD_DIM:(head + 1) * HEAD_DIM] = jnp.transpose(acc_scr[head] / total).astype(BF16)


def attention_chunk(bounds, q_rot, kv_all, first_rows, chunk, rows, kv_local, after):
    tokens = kv_all.shape[0]
    width = q_rot.shape[1] // kv_local
    group = width // HEAD_DIM
    flops = 4 * rows * q_rot.shape[1] * tokens
    return pl.pallas_call(
        functools.partial(attn_kernel, group, chunk),
        out_shape=jax.ShapeDtypeStruct((rows, q_rot.shape[1]), BF16),
        grid_spec=pltpu.PrefetchScalarGridSpec(
            num_scalar_prefetch=1,
            grid=(kv_local,),
            in_specs=[
                pl.BlockSpec((rows, width), lambda g, b: (chunk, g)),
                pl.BlockSpec((tokens, HEAD_DIM), lambda g, b: (0, g)),
                pl.BlockSpec((tokens, HEAD_DIM), lambda g, b: (0, kv_local + g)),
                pl.BlockSpec((1, rows), lambda g, b: (0, chunk)),
            ] + [pl.BlockSpec(memory_space=pl.ANY)] * len(after),
            out_specs=pl.BlockSpec((rows, width), lambda g, b: (0, g)),
            scratch_shapes=[
                pltpu.VMEM((group, HEAD_DIM, rows), BF16),
                pltpu.VMEM((group, 1, rows), F32),
                pltpu.VMEM((group, 8, rows), F32),
                pltpu.VMEM((group, HEAD_DIM, rows), F32),
            ],
        ),
        compiler_params=pltpu.CompilerParams(dimension_semantics=("arbitrary",), vmem_limit_bytes=VMEM_GRANT),
        cost_estimate=pl.CostEstimate(flops=2 * flops, bytes_accessed=2 * kv_all.size, transcendentals=flops // 512),
    )(bounds, q_rot, kv_all, kv_all, first_rows, *after)


def out_proj_kernel(parts, *refs):
    a_refs, (w_ref, x_ref), (o_ref, ssq_ref) = refs[:parts], refs[parts:parts + 2], refs[-2:]
    slabs = w_ref.shape[0]
    acc = None
    for j in range(parts):
        w_cols = jnp.concatenate([w_ref[s, j] for s in range(slabs)], axis=0)
        term = jnp.dot(a_refs[j][...], w_cols, preferred_element_type=F32)
        acc = term if acc is None else acc + term
    total = x_ref[...].astype(F32) + acc
    o_ref[...] = total
    squares = total * total
    part = squares[:, :128]
    for i in range(1, squares.shape[1] // 128):
        part = part + squares[:, i * 128:(i + 1) * 128]

    @pl.when(pl.program_id(0) == 0)
    def _():
        ssq_ref[...] = part

    @pl.when(pl.program_id(0) > 0)
    def _():
        ssq_ref[...] += part


def out_proj(attn_parts, wo_cols, x_cols, chunk, after):
    parts = len(attn_parts)
    rows, depth = attn_parts[0].shape
    slabs, _, slab_rows, cols = wo_cols.shape
    tile = min(OUT_TILE, cols)
    return pl.pallas_call(
        functools.partial(out_proj_kernel, parts),
        out_shape=(jax.ShapeDtypeStruct((rows, cols), F32), jax.ShapeDtypeStruct((rows, 128), F32)),
        grid=(cols // tile,),
        in_specs=[pl.BlockSpec((rows, depth), lambda n: (0, 0))] * parts + [
            pl.BlockSpec((slabs, parts, slab_rows, tile), lambda n: (0, 0, 0, n)),
            pl.BlockSpec((rows, tile), lambda n: (chunk, n)),
        ] + [pl.BlockSpec(memory_space=pl.ANY)] * len(after),
        out_specs=(pl.BlockSpec((rows, tile), lambda n: (0, n)), pl.BlockSpec((rows, 128), lambda n: (0, 0))),
        compiler_params=pltpu.CompilerParams(dimension_semantics=("arbitrary",), vmem_limit_bytes=VMEM_GRANT),
        cost_estimate=pl.CostEstimate(flops=2 * rows * parts * depth * cols, bytes_accessed=2 * wo_cols.size, transcendentals=0),
    )(*attn_parts, wo_cols, x_cols, *after)


def mlp_kernel(parts, rank_ref, *refs):
    u_refs, (wg_ref, wu_ref, wd_ref), o_ref = refs[:parts], refs[parts:parts + 3], refs[-1]
    depth = u_refs[0].shape[1]
    cols = o_ref.shape[2]

    def project(w_ref):
        acc = None
        for j in range(parts):
            owner = lax.rem(rank_ref[0] + j, parts)
            w_rows = w_ref[pl.ds(pl.multiple_of(owner * depth, depth), depth), :]
            term = jnp.dot(u_refs[j][...], w_rows, preferred_element_type=F32)
            acc = term if acc is None else acc + term
        return acc

    hidden = (jax.nn.silu(project(wg_ref)) * project(wu_ref)).astype(BF16)

    @pl.when(pl.program_id(0) == 0)
    def _():
        for j in range(o_ref.shape[0]):
            o_ref[j] = jnp.dot(hidden, wd_ref[:, j * cols:(j + 1) * cols], preferred_element_type=F32)

    @pl.when(pl.program_id(0) > 0)
    def _():
        for j in range(o_ref.shape[0]):
            o_ref[j] += jnp.dot(hidden, wd_ref[:, j * cols:(j + 1) * cols], preferred_element_type=F32)


def mlp_partial(rank, u_parts, w_gate, w_up, w_down, after):
    if isinstance(u_parts, list):
        parts = len(u_parts)
        rows, depth = u_parts[0].shape
        u_specs = [pl.BlockSpec((rows, depth), lambda i, r: (0, 0))] * parts
    else:
        parts, rows, depth = u_parts.shape
        u_specs = [pl.BlockSpec((None, rows, depth), lambda i, r, j=j: (j, 0, 0)) for j in range(parts)]
        u_parts = [u_parts] * parts
    ff_local = w_gate.shape[1]
    tile = FF_TILE
    model = w_down.shape[1]
    return pl.pallas_call(
        functools.partial(mlp_kernel, parts),
        out_shape=jax.ShapeDtypeStruct((parts, rows, model // parts), F32),
        grid_spec=pltpu.PrefetchScalarGridSpec(
            num_scalar_prefetch=1,
            grid=(ff_local // tile,),
            in_specs=u_specs + [
                pl.BlockSpec((parts * depth, tile), lambda i, r: (0, i)),
                pl.BlockSpec((parts * depth, tile), lambda i, r: (0, i)),
                pl.BlockSpec((tile, model), lambda i, r: (i, 0)),
            ] + [pl.BlockSpec(memory_space=pl.ANY)] * len(after),
            out_specs=pl.BlockSpec((parts, rows, model // parts), lambda i, r: (0, 0, 0)),
        ),
        compiler_params=pltpu.CompilerParams(dimension_semantics=("arbitrary",), vmem_limit_bytes=VMEM_GRANT),
        cost_estimate=pl.CostEstimate(flops=6 * rows * model * ff_local, bytes_accessed=6 * model * ff_local,
                                      transcendentals=rows * ff_local),
    )(rank, *u_parts, w_gate, w_up, w_down, *after)


def join_kernel(parts, rank_ref, *refs):
    part_refs, o_ref = refs[:parts], refs[-1]
    cols = part_refs[0].shape[1]
    for j in range(parts):
        owner = lax.rem(rank_ref[0] + j, parts)
        o_ref[:, pl.ds(pl.multiple_of(owner * cols, cols), cols)] = part_refs[j][...]


def join(rank, y_parts, y_out, chunk, chunks):
    parts = len(y_parts)
    rows, cols = y_parts[0].shape
    in_specs = [pl.BlockSpec((rows, cols), lambda i, r: (0, 0))] * parts
    operands = [rank, *y_parts]
    aliases = {}
    if y_out is not None:
        aliases = {len(operands): 0}
        in_specs = in_specs + [pl.BlockSpec(memory_space=pl.ANY)]
        operands.append(y_out)
    return pl.pallas_call(
        functools.partial(join_kernel, parts),
        out_shape=jax.ShapeDtypeStruct((rows * chunks, parts * cols), BF16),
        grid_spec=pltpu.PrefetchScalarGridSpec(
            num_scalar_prefetch=1,
            grid=(1,),
            in_specs=in_specs,
            out_specs=pl.BlockSpec((rows, parts * cols), lambda i, r: (chunk, 0)),
        ),
        input_output_aliases=aliases,
        compiler_params=pltpu.CompilerParams(dimension_semantics=("arbitrary",), vmem_limit_bytes=VMEM_GRANT),
        cost_estimate=pl.CostEstimate(flops=0, bytes_accessed=4 * rows * parts * cols, transcendentals=0),
    )(*operands)


def ring_gather(own, axis, size, forward):
    def shifted(block, shift):
        return lax.ppermute(block, axis, [(i, (i + shift) % size) for i in range(size)])

    if size != 4:
        return [own] + [shifted(own, -k) for k in range(1, size)]
    before = shifted(own, 1)
    behind = shifted(own, -1)
    opposite = shifted(before, 1) if forward else shifted(behind, -1)
    return [own, behind, opposite, before]


def pipeline_order(chunks):
    order = [("attn", chunk) for chunk in range(chunks - 1)]
    order += [("out", chunk) for chunk in range(chunks - 2)]
    order += [("attn", chunks - 1), ("mlp", 0), ("out", chunks - 2), ("out", chunks - 1)]
    return order + [("mlp", chunk) for chunk in range(1, chunks)]


def solution(mesh):
    sp_size = mesh.shape["sp"]
    tp_size = mesh.shape["tp"]
    row_spec = P(("rep", "sp"), None)
    tok_spec = P(("rep", "sp"))
    full_spec = P(None)
    col_spec = P(None, "tp")
    wrow_spec = P("tp", None)
    cache_spec = P("rep", ("tp", "sp"), None)

    def local_layer(x_in, positions, segments, gain_attn, w_q, w_k, w_v, w_o, gain_mlp, w_gate, w_up, w_down):
        rows_local, model = x_in.shape
        kv_local = w_k.shape[1] // HEAD_DIM
        heads_local = w_q.shape[1] // HEAD_DIM
        kv_repeat = sp_size // kv_local
        rows = rows_local // CHUNKS
        cols = model // tp_size
        sp_rank = lax.axis_index("sp")
        tp_rank = lax.axis_index("tp")
        row_base = sp_rank * rows_local

        below = jnp.sum(segments[:, None] < jnp.arange(NUM_REQS)[None, :], axis=0, dtype=jnp.int32)
        starts = lax.psum(below, "sp")
        first_rows = jnp.sum(jnp.where(segments[:, None] == jnp.arange(NUM_REQS)[None, :], starts[None, :], 0), axis=1,
                             dtype=jnp.int32)

        x_f32 = x_in.astype(F32)
        u_norm = rms_norm(x_f32, gain_attn)
        cos_t, sin_t = rope_tables(positions)
        k_rot = rotate(jnp.dot(u_norm, w_k, preferred_element_type=F32).reshape(rows_local, -1, HEAD_DIM), cos_t, sin_t).astype(BF16)
        v_proj = jnp.dot(u_norm, w_v, preferred_element_type=F32).astype(BF16)
        kv_own = jnp.concatenate([k_rot.reshape(rows_local, -1), v_proj], axis=1)
        kv_all = lax.all_gather(kv_own, "sp", tiled=True)
        q_raw = jnp.dot(u_norm, w_q, preferred_element_type=F32)
        q_rot = rotate(q_raw.reshape(rows_local, -1, HEAD_DIM), cos_t, sin_t).astype(BF16)
        q_rot = q_rot.reshape(rows_local, -1)
        slot_head = sp_rank // kv_repeat
        k_cache = lax.dynamic_slice_in_dim(kv_all, slot_head * HEAD_DIM, HEAD_DIM, axis=1)[:, None, :]
        v_cache = lax.dynamic_slice_in_dim(kv_all, (kv_local + slot_head) * HEAD_DIM, HEAD_DIM, axis=1)[:, None, :]

        slab_rows = heads_local * HEAD_DIM // sp_size
        slab = lax.dynamic_slice_in_dim(w_o, sp_rank * slab_rows, slab_rows, axis=0)
        slabs = [lax.dynamic_slice_in_dim(slab, tp_rank * cols, cols, axis=1)]
        for k in range(1, tp_size):
            block = lax.dynamic_slice_in_dim(slab, lax.rem(tp_rank + tp_size - k, tp_size) * cols, cols, axis=1)
            slabs.append(lax.ppermute(block, "tp", [(i, (i + tp_size - k) % tp_size) for i in range(tp_size)]))
        wo_cols = lax.all_gather(jnp.stack(slabs), "sp")
        x_cols = lax.dynamic_slice_in_dim(x_in, tp_rank * cols, cols, axis=1)
        gain_cols = lax.dynamic_slice_in_dim(gain_mlp, tp_rank * cols, cols, axis=0)

        rank = jnp.reshape(tp_rank, (1,)).astype(jnp.int32)
        rank_zero = jnp.zeros((1,), jnp.int32)
        bounds = jnp.stack([row_base + chunk * rows + jnp.zeros((), jnp.int32) if part == 0 else
                            first_rows[chunk * rows + (part - 1) * (rows - 1)]
                            for chunk in range(CHUNKS) for part in range(3)])

        def near(parts):
            return [parts[1], parts[-1]]

        attn_all, x_mid, u_all, y_own, y_all, row_sq = {}, {}, {}, {}, {}, {}
        after = [q_rot]
        for stage, chunk in pipeline_order(CHUNKS):
            forward = chunk % 2 == 0
            if stage == "attn":
                if chunk >= 2:
                    after = after + near(attn_all[chunk - 2])
                attn_own = attention_chunk(bounds, q_rot, kv_all, first_rows[None, :], chunk, rows, kv_local, after)
                attn_all[chunk] = ring_gather(attn_own, "tp", tp_size, forward)
                after = [attn_own]
            elif stage == "out":
                if chunk == CHUNKS - 2:
                    after = after + near(attn_all[CHUNKS - 1])
                x_mid[chunk], ssq = out_proj(attn_all[chunk], wo_cols, x_cols, chunk, after)
                row_sq[chunk] = jnp.sum(ssq, axis=1)
                after = [x_mid[chunk]]
                if chunk % 2 == 1:
                    pair = (chunk - 1, chunk)
                    sums = lax.psum(jnp.concatenate([row_sq[c] for c in pair]), "tp")
                    after = []
                    for place, c in enumerate(pair):
                        sum_sq = sums[place * rows:(place + 1) * rows]
                        u_own = (x_mid[c] * lax.rsqrt(sum_sq[:, None] / model + NORM_EPS) * gain_cols).astype(BF16)
                        if c == 0:
                            u_all[c] = lax.all_gather(u_own, "tp")
                        else:
                            u_all[c] = ring_gather(u_own, "tp", tp_size, c % 2 == 0)
                        after.append(u_own)
            else:
                if chunk == 0:
                    after = after + near(u_all[1]) + near(attn_all[CHUNKS - 2])
                if chunk >= 2:
                    after = after + [y_own[chunk - 2]]
                    if chunk + 1 < CHUNKS:
                        after = after + near(u_all[chunk + 1])
                if chunk >= 3:
                    after = after + near(y_all[chunk - 3])
                own_rank = rank if isinstance(u_all[chunk], list) else rank_zero
                partial = mlp_partial(own_rank, u_all[chunk], w_gate, w_up, w_down, after)
                down = lax.psum_scatter(partial, "tp", scatter_dimension=0, tiled=False)
                y_own[chunk] = (x_mid[chunk] + down).astype(BF16)
                y_all[chunk] = ring_gather(y_own[chunk], "tp", tp_size, forward)
                after = [partial]
        y_out = None
        for chunk in range(CHUNKS):
            y_out = join(rank, y_all[chunk], y_out, chunk, CHUNKS)
        return y_out, k_cache, v_cache

    return jax.shard_map(local_layer, mesh=mesh,
                         in_specs=(row_spec, tok_spec, tok_spec, full_spec, col_spec, col_spec, col_spec, wrow_spec,
                                   full_spec, col_spec, col_spec, wrow_spec),
                         out_specs=(row_spec, cache_spec, cache_spec), check_vma=False)
```
